32 devices in a mesh: mem: 8 (over z, y), hz: 4 (over x, core).
Axes of the slice: x: 2, y: 2, z: 4, core: 2. Of those that a mesh axis runs over, the one named last changes fastest.
Arguments:
- prior: float32 [8, 64, 32768], P('mem', None, 'hz'), may hold values from -6 to 6
- posterior: float32 [8, 64, 32768], P('mem', None, 'hz'), may hold values from -4 to 4
- control: float32 [64, 32768], P(None, 'hz'), may hold values from -6 to 6
- relax: float32 [64], replicated, may hold values from 0.5 to 0.95
- ocean: int32 [32768], P('hz'), may hold values 0 or 1
Outputs:
- analysis: float32 [8, 64, 32768], P('mem', None, 'hz')
The draws below stay inside these ranges and needn't reach their ends.
All inputs are finite; a program needn't handle non-finite values. No bound on the sum of `ocean` on one device may be relied on, other than what follows from the above.
Results may differ from the reference program's by a relative error of at most 0.00002.
Values sent between devices are 32-bit elements; how exact they have to be, the bound alone decides.
No kernel may reach another device: no remote copies, remote signals or barrier semaphores. Data moves between devices by JAX's collectives and lax.ppermute only.
A program may use at most 64 MiB of HBM per device.

```python
import jax
import jax.numpy as jnp
from jax import lax

LEV = 64
MEMBERS = 8
NCOL = 32768


def touch_ends(drawn, rng, low, largest):
    dims = drawn.shape
    spot = [jax.random.randint(jax.random.fold_in(rng, axis), (), 0, dims[axis]) for axis in range(len(dims))]
    drawn = drawn.at[tuple(spot)].set(low)
    longest = dims.index(max(dims))
    spot[longest] = (spot[longest] + 1) % dims[longest]
    return drawn.at[tuple(spot)].set(largest)


def block_scale(key, shape, cuts, low, largest):
    def one(position, parts):
        draws = jax.random.uniform(jax.random.fold_in(jax.random.fold_in(key, 6), position), (parts,), jnp.float32, low / len(cuts), largest / len(cuts))
        return jnp.repeat(jnp.exp(draws), shape[position] // parts).reshape((-1,) + (1,) * (len(shape) - position - 1))

    loudness = one(*cuts[0])
    for cut in cuts[1:]:
        loudness = loudness * one(*cut)
    return loudness


def centred(key, dims, width, reach, shards=(), held_as=jnp.bfloat16):
    array = width * jax.random.normal(key, dims, jnp.float32)
    if shards:
        array = array * block_scale(key, dims, shards, -0.22, 0.18)
    return jnp.clip(array, -reach, reach).astype(held_as)


def setup_inputs(seed: int = 0) -> dict:
    key_of = jax.random.split(jax.random.key(seed), 6)
    prior = centred(key_of[0], (MEMBERS, LEV, NCOL), 1.0, 6.0, ((0, 8), (2, 4)), jnp.float32)
    posterior = centred(key_of[1], (MEMBERS, LEV, NCOL), 0.6, 4.0, ((0, 8), (2, 4)), jnp.float32)
    control = centred(key_of[2], (LEV, NCOL), 1.0, 6.0, ((1, 4),), jnp.float32)
    relax = jnp.clip(jax.random.uniform(key_of[3], (LEV,), jnp.float32, 0.5, 0.95), 0.5, 0.95)
    ocean = touch_ends((jax.random.randint(key_of[4], (NCOL,), 0, 4) < 3).astype(jnp.int32), jax.random.fold_in(key_of[4], 1), 0, 1)
    return {"prior": prior, "posterior": posterior, "control": control, "relax": relax, "ocean": ocean}


eps = 1e-06

def reference(prior, posterior, control, relax, ocean):
    prior_mean = lax.optimization_barrier(jnp.sum(prior, axis=0)) / MEMBERS
    post_mean = lax.optimization_barrier(jnp.sum(posterior, axis=0)) / MEMBERS
    weights = ocean.astype(jnp.float32)
    prior_anom = prior - prior_mean
    post_anom = posterior - post_mean
    prior_spread = lax.optimization_barrier(jnp.sum(prior_anom * prior_anom * weights, axis=(0, 2)))
    post_spread = lax.optimization_barrier(jnp.sum(post_anom * post_anom * weights, axis=(0, 2)))
    factor = relax * (jnp.sqrt((prior_spread + eps) / (post_spread + eps)) - 1.0) + 1.0
    return control + factor[None, :, None] * post_anom
```

```python
import jax
import jax.numpy as jnp
from jax import lax
from jax.sharding import PartitionSpec as P

eps = 1e-06
CHUNKS = 2
LANES = 128


def inflation(relax, prior_spread, post_spread):
    return relax * (jnp.sqrt((prior_spread + eps) / (post_spread + eps)) - 1.0) + 1.0


def halves(x):
    w = x.shape[-1] // 2
    return x[..., :w], x[..., w:]


def on_device(prior, posterior, control, relax, ocean):
    n = lax.axis_size("mem")
    me = lax.axis_index("mem")
    members = prior.shape[0] * n
    columns = prior.shape[2]
    steps = [1 << k for k in range(n.bit_length() - 1)]
    chunks = max(1, min(CHUNKS, columns // (n * LANES)))
    width = columns // chunks
    weights = ocean.astype(jnp.float32)[None, :]

    def upper(step):
        return (me // step) % 2 == 1

    def swap(x, step):
        return lax.ppermute(x, "mem", [(i, i ^ step) for i in range(n)])

    def keep(x, step):
        low, high = halves(x)
        return jnp.where(upper(step), high, low)

    def give(x, step):
        low, high = halves(x)
        return jnp.where(upper(step), low, high)

    def part(x, c):
        return x[..., c * width:(c + 1) * width]

    def scatter(x):
        for step in steps:
            x = keep(x, step) + swap(give(x, step), step)
        return x

    def gather(x):
        for step in reversed(steps):
            other = swap(x, step)
            x = jnp.where(
                upper(step), jnp.concatenate([other, x], axis=1), jnp.concatenate([x, other], axis=1)
            )
        return x

    post = jnp.sum(posterior, axis=0)
    prio = jnp.sum(prior, axis=0)
    post_piece = [scatter(part(post, c)) for c in range(chunks)]
    prio_piece = [scatter(part(prio, c)) for c in range(chunks)]
    held = []
    for c in range(chunks):
        w = part(weights, c)
        for step in steps:
            w = keep(w, step)
        held.append(w)

    def local(x, pieces):
        total = jnp.sum(x * x * weights, axis=(0, 2))
        for piece, w in zip(pieces, held):
            total = total - jnp.sum(piece * piece * w, axis=1) / members
        return total

    spread = lax.psum(jnp.stack([local(prior, prio_piece), local(posterior, post_piece)]), ("mem", "hz"))
    factor = inflation(relax, spread[0], spread[1])
    mean = jnp.concatenate([gather(x) for x in post_piece], axis=1) / members
    return control + factor[None, :, None] * (posterior - mean)


def solution(mesh):
    return jax.shard_map(
        on_device,
        mesh=mesh,
        in_specs=(P("mem", None, "hz"), P("mem", None, "hz"), P(None, "hz"), P(), P("hz")),
        out_specs=P("mem", None, "hz"),
        check_vma=False,
    )
```

```python
import jax
import jax.numpy as jnp
from jax import lax
from jax.sharding import PartitionSpec as P

eps = 1e-06
CHUNKS = 2
LANES = 128


def inflation(relax, prior_spread, post_spread):
    return relax * (jnp.sqrt((prior_spread + eps) / (post_spread + eps)) - 1.0) + 1.0


def after(x, *others):
    return lax.optimization_barrier((x,) + others)[0]


def halves(x):
    w = x.shape[-1] // 2
    return x[..., :w], x[..., w:]


def xor_steps(axis):
    return [1 << k for k in range(lax.axis_size(axis).bit_length() - 1)]


def swap(x, axis, step):
    return lax.ppermute(x, axis, [(i, i ^ step) for i in range(lax.axis_size(axis))])


def on_device(prior, posterior, control, relax, ocean):
    n = lax.axis_size("mem")
    me = lax.axis_index("mem")
    members = prior.shape[0] * n
    columns = prior.shape[2]
    steps = xor_steps("mem")
    near_last = steps[1:] + steps[:1]
    chunks = max(1, min(CHUNKS, columns // (n * LANES)))
    width = columns // chunks
    weights = ocean.astype(jnp.float32)[None, :]

    def upper(step):
        return (me & step) != 0

    def keep(x, step):
        low, high = halves(x)
        return jnp.where(upper(step), high, low)

    def give(x, step):
        low, high = halves(x)
        return jnp.where(upper(step), low, high)

    def part(x, c):
        return x[..., c * width:(c + 1) * width]

    def scatter(x, order):
        for step in order:
            x = keep(x, step) + swap(give(x, step), "mem", step)
        return x

    def gather(x, order):
        for step in reversed(order):
            other = swap(x, "mem", step)
            x = jnp.where(
                upper(step), jnp.concatenate([other, x], axis=1), jnp.concatenate([x, other], axis=1)
            )
        return x

    def first(x, c, order, sent_after, kept_after):
        step = order[0]
        sent = give(part(x, c), step)
        got = swap(after(sent, *sent_after), "mem", step)
        mine = keep(part(after(x, *kept_after), c), step)
        return got, mine + got

    post = jnp.sum(posterior, axis=0)
    prio = jnp.sum(prior, axis=0)

    post_order = [steps] * chunks
    prio_order = [steps if c + 1 < chunks or chunks == 1 else near_last for c in range(chunks)]

    post_half, post_got = [], []
    done = ()
    for c in range(chunks):
        got, x = first(post, c, post_order[c], (), done)
        done = (x,)
        post_got.append(got)
        post_half.append(x)
    prio_half = [None] * chunks
    done = ()
    for c in reversed(range(chunks)):
        gate = () if prio_order[c] is near_last else (post_got[0],)
        got, x = first(prio, c, prio_order[c], gate, done)
        done = (x,)
        prio_half[c] = x
    post_piece = [scatter(x, o[1:]) for x, o in zip(post_half, post_order)]
    prio_piece = [scatter(x, o[1:]) for x, o in zip(prio_half, prio_order)]

    def local(x, pieces, orders):
        total = jnp.sum(x * x * weights, axis=(0, 2))
        for c, (piece, order) in enumerate(zip(pieces, orders)):
            w = part(weights, c)
            for step in order:
                w = keep(w, step)
            total = total - jnp.sum(piece * piece * w, axis=1) / members
        return total

    spread = jnp.stack([local(prior, prio_piece, prio_order), local(posterior, post_piece, post_order)])
    for axis in ("hz", "mem"):
        for step in xor_steps(axis):
            spread = spread + swap(spread, axis, step)
    factor = inflation(relax, spread[0], spread[1])
    mean = jnp.concatenate([gather(x, o) for x, o in zip(post_piece, post_order)], axis=1) / members
    return control + factor[None, :, None] * (posterior - mean)


def solution(mesh):
    return jax.shard_map(
        on_device,
        mesh=mesh,
        in_specs=(P("mem", None, "hz"), P("mem", None, "hz"), P(None, "hz"), P(), P("hz")),
        out_specs=P("mem", None, "hz"),
        check_vma=False,
    )
```
